256 devices in a mesh: groups: 2 (over z), seq: 64 (over x, y), mp: 2 (over core).
Axes of the slice: x: 8, y: 8, z: 2, core: 2. Of those that a mesh axis runs over, the one named last changes fastest.
The devices are a block of a 8x8x16 slice.
Arguments:
- latent_cache: bfloat16 [16384, 64, 512], P(('groups', 'seq')), parts along dimension 0, may hold values from -6 to 6
- rope_cache: bfloat16 [16384, 4096], P(('groups', 'seq')), parts along dimension 0, may hold values from -6 to 6
- q_nope: bfloat16 [16, 128, 128], P('groups', 'mp'), parts along dimension 0, may hold values from -12 to 12
- q_rope: bfloat16 [16, 128, 64], P('groups', 'mp'), parts along dimension 0, may hold values from -2000 to 2000
- w_uk: bfloat16 [128, 128, 512], P('mp', None, 'seq'), may hold values from -0.5 to 0.5
- value_up_weight: bfloat16 [128, 512, 128], P('mp', 'seq'), may hold values from -0.25 to 0.25
- w_out: bfloat16 [16384, 7168], P('mp', 'seq'), may hold values from -0.046875 to 0.046875
- page_table: int32 [16, 2048], P('groups'), parts along dimension 0, may hold values from 0 to 8191, as said below
- lengths: int32 [16], P('groups'), parts along dimension 0, may hold values from 16384 to 131072, as said below
Outputs:
- output: bfloat16 [16, 7168], P('groups', ('seq', 'mp')), parts along dimension 0
The draws below stay inside these ranges and needn't reach their ends.
There are 2 independent parts, one for each index of `groups`. The reference program is written for one: setup_inputs(seed, part) draws one part's arguments, and reference() takes and returns one part's arrays. A program takes and returns all parts, laid end to end along the dimension named above; an argument that names none is the same for every part. Nothing has to cross between parts.
Inputs may be any that keep to these rules, and one draw needn't show every extreme that they name: `lengths`: every sequence has one eighth of 131072 tokens or more; the longest has exactly 131072. page_table[b,p] for p < ceil(lengths[b] / 64) is the global slot (shard index times 128 plus local slot) holding that page; these live entries are all distinct; the other entries are 0 and unused.
All inputs are finite; a program needn't handle non-finite values.
Results may differ from the reference program's by a relative error of at most 0.012.
Values may be sent and summed in bfloat16 or wider, within the bound.
A program may use at most 64 MiB of HBM per device.

```python
import jax
import jax.numpy as jnp
from jax import lax

B = 8
H = 128
NOPE = 128
ROPE = 64
KVR = 512
VDIM = 128
D = 7168
PAGE = 64
SLOTS_DEV = 128
SLOTS = 8192
MAXLEN = 131072
MAXPAGES = 2048
N_SEQ = 64


def page_layout(key):
    key_len, key_long, key_weight, key_perm = jax.random.split(jax.random.fold_in(key, 11), 4)
    others = jax.random.randint(key_len, (B,), MAXLEN // 8, MAXLEN // 4 + 1)
    longest_length = jax.random.randint(key_long, (), 0, B)
    lengths = jnp.where(jnp.arange(B) == longest_length, MAXLEN, others).astype(jnp.int32)
    page_count = (lengths + PAGE - 1) // PAGE
    offsets = jnp.cumsum(page_count) - page_count
    weight = jax.random.randint(key_weight, (N_SEQ,), 0, 4)
    shuffled = jax.random.permutation(key_perm, SLOTS)
    ranking = jnp.repeat(weight, SLOTS_DEV) * SLOTS + shuffled
    slot_order = jnp.argsort(-ranking)
    logical = jnp.arange(MAXPAGES)
    position = jnp.clip(offsets[:, None] + logical[None, :], 0, SLOTS - 1)
    page_map = jnp.where(logical[None, :] < page_count[:, None], slot_order[position], 0).astype(jnp.int32)
    return (lengths, page_map)


def rope_values(key):
    base = jnp.clip(jax.random.normal(jax.random.fold_in(key, 23), (SLOTS, PAGE, ROPE), jnp.float32), -6.0, 6.0)
    return base


def draw_lengths(key, part):
    return page_layout(key)[0]


def draw_page_table(key, part):
    return page_layout(key)[1]


def draw_rope_cache(key, part):
    return rope_values(key).reshape(SLOTS, PAGE * ROPE).astype(jnp.bfloat16)


def draw_q_rope(key, part):
    drawn = jnp.clip(2.0 * jax.random.normal(jax.random.fold_in(key, 31), (B, H, ROPE), jnp.float32), -12.0, 12.0)
    return drawn.astype(jnp.bfloat16)


def steps_of(key, dims, shards, low, high):
    gain, own = 1.0, jax.random.fold_in(key, 6)
    for dim, blocks in shards:
        steps = jnp.exp(jax.random.uniform(jax.random.fold_in(own, dim), (blocks,), jnp.float32, low / len(shards), high / len(shards)))
        gain = gain * jnp.repeat(steps, dims[dim] // blocks).reshape([-1 if axis == dim else 1 for axis in range(len(dims))])
    return gain


def gaussian(rng, extent, deviation, limit, cuts=(), held_as=jnp.bfloat16):
    gain = steps_of(rng, extent, cuts, -0.22, 0.18) if cuts else 1.0
    values = jax.random.normal(rng, extent, jnp.float32) * deviation * gain
    return jnp.minimum(jnp.maximum(values, -limit), limit).astype(held_as)


def setup_inputs(seed: int = 0, part: int = 0) -> dict:
    splits = jax.random.split(jax.random.key(seed), 10)
    part_keys = jax.random.split(jax.random.fold_in(splits[9], part), 10)
    latent_cache = gaussian(part_keys[0], (SLOTS, PAGE, KVR), 1.0, 6.0, ((0, 64),))
    rope_cache = draw_rope_cache(jax.random.fold_in(jax.random.fold_in(splits[9], part), 71), part)
    q_nope = gaussian(part_keys[2], (B, H, NOPE), 2.0, 12.0, ((1, 2),))
    q_rope = draw_q_rope(jax.random.fold_in(jax.random.fold_in(splits[9], part), 71), part)
    w_uk = gaussian(splits[4], (H, NOPE, KVR), NOPE ** -0.5, 0.5, ((0, 2), (2, 64)))
    value_up_weight = gaussian(splits[5], (H, KVR, VDIM), KVR ** -0.5, 0.25, ((0, 2), (1, 64)))
    w_out = gaussian(splits[6], (H * VDIM, D), (H * VDIM) ** -0.5, 0.046875, ((0, 2), (1, 64)))
    page_table = draw_page_table(jax.random.fold_in(jax.random.fold_in(splits[9], part), 71), part)
    lengths = draw_lengths(jax.random.fold_in(jax.random.fold_in(splits[9], part), 71), part)
    return dict(latent_cache=latent_cache, rope_cache=rope_cache, q_nope=q_nope, q_rope=q_rope, w_uk=w_uk, value_up_weight=value_up_weight, w_out=w_out, page_table=page_table, lengths=lengths)


NEG = -1.0e30


def reference(latent_cache, rope_cache, q_nope, q_rope, w_uk, value_up_weight, w_out, page_table, lengths):
    score_scale = (NOPE + ROPE) ** -0.5
    peak_score = lax.Precision.HIGHEST
    q_latent = jnp.einsum('bhn,hnk->bhk', q_nope.astype(jnp.float32), w_uk.astype(jnp.float32), precision=peak_score).astype(jnp.bfloat16)
    page_count = (lengths + PAGE - 1) // PAGE
    logical = jnp.arange(MAXPAGES, dtype=jnp.int32)
    live_page = logical[None, :] < page_count[:, None]
    tokens_in = jnp.clip(lengths[:, None] - PAGE * logical[None, :], 0, PAGE).astype(jnp.int32)
    target = jnp.where(live_page, page_table, SLOTS).astype(jnp.int32).reshape(-1)
    seq_ids = jnp.broadcast_to(jnp.arange(B, dtype=jnp.int32)[:, None], (B, MAXPAGES)).reshape(-1)
    slot_owner = jnp.zeros((SLOTS, B), jnp.float32).at[target, seq_ids].set(1.0, mode='drop')
    slot_fill = jnp.zeros((SLOTS,), jnp.int32).at[target].add(tokens_in.reshape(-1), mode='drop')
    blocks = SLOTS // 8
    latent_blocks = latent_cache.reshape(blocks, 8, PAGE, KVR)
    rope_blocks = rope_cache.reshape(blocks, 8, PAGE, ROPE)
    owner_blocks = slot_owner.reshape(blocks, 8, B)
    fill_blocks = slot_fill.reshape(blocks, 8)
    q_latent_f = q_latent.astype(jnp.float32)
    q_rope_f = q_rope.astype(jnp.float32)

    def step_block(run_state, block_data):
        run_max, run_sum, run_out = run_state
        latent_block, rope_block, owner_block, fill_block = block_data
        latent_f = latent_block.astype(jnp.float32)
        pick_latent = jnp.einsum('sb,bhk->shk', owner_block, q_latent_f, precision=peak_score)
        pick_rope = jnp.einsum('sb,bhr->shr', owner_block, q_rope_f, precision=peak_score)
        scores = (jnp.einsum('shk,stk->sht', pick_latent, latent_f, precision=peak_score)
                  + jnp.einsum('shr,str->sht', pick_rope, rope_block.astype(jnp.float32), precision=peak_score)) * score_scale
        live_token = jnp.arange(PAGE, dtype=jnp.int32)[None, None, :] < fill_block[:, None, None]
        slot_max = jnp.max(jnp.where(live_token, scores, NEG), axis=2)
        exponent = jnp.where(live_token, jnp.exp(scores - slot_max[:, :, None]), 0.0)
        slot_sum = jnp.sum(exponent, axis=2)
        weights = lax.optimization_barrier(exponent.astype(jnp.bfloat16)).astype(jnp.float32)
        slot_out = jnp.einsum('sht,stk->shk', weights, latent_f, precision=peak_score)
        owned = jnp.transpose(owner_block) > 0
        candidate = jnp.where(owned[:, :, None], slot_max[None, :, :], NEG)
        new_max = jnp.maximum(run_max, jnp.max(candidate, axis=1))
        carry_scale = jnp.exp(run_max - new_max)
        factor = jnp.where(owned[:, :, None], jnp.exp(candidate - new_max[:, None, :]), 0.0)
        run_sum = run_sum * carry_scale + jnp.einsum('bsh,sh->bh', factor, slot_sum, precision=peak_score)
        run_out = run_out * carry_scale[:, :, None] + jnp.einsum('bsh,shk->bhk', factor, slot_out, precision=peak_score)
        return (new_max, run_sum, run_out), None

    initial = (jnp.full((B, H), NEG, jnp.float32), jnp.zeros((B, H), jnp.float32), jnp.zeros((B, H, KVR), jnp.float32))
    final_state, unused = lax.scan(step_block, initial, (latent_blocks, rope_blocks, owner_blocks, fill_blocks))
    seq_max, seq_sum, seq_out = final_state
    attention_probs = (seq_out / seq_sum[:, :, None]).astype(jnp.bfloat16)
    value_rows = jnp.einsum('gre,req->grq', attention_probs.astype(jnp.float32), value_up_weight.astype(jnp.float32), precision=peak_score).astype(jnp.bfloat16)
    output = jnp.dot(value_rows.reshape(B, H * VDIM), w_out, preferred_element_type=jnp.float32).astype(jnp.bfloat16)
    return output
```

```python
import functools
import math

import jax
import jax.numpy as jnp
from jax import lax
from jax.experimental import pallas as pl
from jax.experimental.pallas import tpu as pltpu
from jax.sharding import PartitionSpec as P

GROUPS_SEQ = ("groups", "seq")
NEG = -1e30
F32 = jnp.float32
BF16 = jnp.bfloat16
NT = (((1,), (1,)), ((), ()))
NN = (((1,), (0,)), ((), ()))


def dot(a, b, dims):
    return lax.dot_general(a, b, dims, preferred_element_type=F32)


def kernel(
    side,
    scale,
    q_nope,
    q_rope,
    w_uk,
    w_up,
    table,
    lengths,
    latent_hbm,
    rope_hbm,
    w_out_hbm,
    out,
    lat,
    rope,
    wout,
    spread,
    keys,
    q_all,
    g0,
    g1,
    wb1,
    wb2,
    fills,
    owner_v,
    owner_s,
    sc,
    mrow,
    lrow,
    probs,
    acc,
    mtile,
    mx,
    mt2,
    my,
    ltile,
    lx,
    lt2,
    ly,
    sx,
    sy,
    rx,
    ry,
    stage,
    r0,
    r1,
    s2y,
    s2x,
    r2y,
    r2x,
    vals,
    part_send,
    part_recv,
    load_sem,
    own_sem,
    send_sem,
    recv_sem,
    mp_sem,
):
    seqs, heads, nope = q_nope.shape
    slots, page, width = lat.shape
    half = seqs * heads // 2
    hw = width // 2
    me = lax.axis_index("seq")
    mp = lax.axis_index("mp")
    x, y = lax.div(me, side), lax.rem(me, side)
    hops = sorted(range(1, side), key=lambda k: -min(k, side - k))

    def to_x(k):
        return lax.rem(x + k, side)

    def to_y(k):
        return lax.rem(y + k, side)

    def at_x(k):
        return {"seq": to_x(k) * side + y}

    def at_y(k):
        return {"seq": x * side + to_y(k)}

    loads = []
    n_cut = 4
    cut = slots // n_cut

    def load(src, dst):
        copy = pltpu.make_async_copy(src, dst, load_sem.at[len(loads)])
        copy.start()
        loads.append(copy)

    load(rope_hbm, rope)
    for i in range(n_cut):
        load(latent_hbm.at[pl.ds(i * cut, cut)], lat.at[pl.ds(i * cut, cut)])
    load(w_out_hbm, wout)

    barrier = pltpu.get_barrier_semaphore()
    for k in hops:
        pl.semaphore_signal(barrier, inc=1, device_id=at_x(k), device_id_type=pl.DeviceIdType.MESH)
        pl.semaphore_signal(barrier, inc=1, device_id=at_y(k), device_id_type=pl.DeviceIdType.MESH)
    pl.semaphore_signal(
        barrier, inc=1, device_id={"mp": 1 - mp}, device_id_type=pl.DeviceIdType.MESH
    )

    started = []

    def send(phase, k, src, dst, device):
        copy = pltpu.make_async_remote_copy(
            src_ref=src,
            dst_ref=dst,
            send_sem=send_sem.at[phase, k],
            recv_sem=recv_sem.at[phase, k],
            device_id=device,
            device_id_type=pl.DeviceIdType.MESH,
        )
        copy.start()
        started.append(copy)
        return copy

    def arrive(copies):
        for copy in copies:
            copy.wait_recv()

    cols = w_uk.shape[1]
    wide = dot(
        w_uk[...].reshape(heads * cols, nope), q_nope[...].reshape(seqs * heads, nope), NT
    ).reshape(heads, cols, seqs * heads)
    row_head = lax.broadcasted_iota(jnp.int32, wide.shape, 0)
    col_head = lax.rem(lax.broadcasted_iota(jnp.int32, wide.shape, 2), heads)
    q_part = jnp.sum(jnp.where(row_head == col_head, wide, 0.0), axis=0).astype(BF16)
    g0[x, y] = q_part[:, :half]
    g1[y, x] = q_part[:, half:]

    pl.semaphore_wait(barrier, 2 * (side - 1) + 1)

    first0 = [send(0, k, g0.at[x, y], g0.at[x, y], at_y(k)) for k in hops]
    first1 = [send(1, k, g1.at[y, x], g1.at[y, x], at_x(k)) for k in hops]

    lane = lax.broadcasted_iota(jnp.int32, (1, 128), 1)
    low = lane < page
    pitch = spread.shape[0] // slots
    rope_copy, lat_copies, wout_copy = loads[0], loads[1:-1], loads[-1]
    rope_copy.wait()

    def spread_pair(c, carry):
        z = rope[:, pl.ds(pl.multiple_of(c * 128, 128), 128)].astype(F32)
        spread[pl.ds(2 * c, slots, stride=pitch), :] = jnp.where(low, z, 0.0)
        spread[pl.ds(2 * c + 1, slots, stride=pitch), :] = jnp.where(low, 0.0, z)
        return carry

    lax.fori_loop(0, rope.shape[1] // 128, spread_pair, 0)

    arrive(first0)
    arrive(first1)
    second0 = [send(2, k, g0.at[x], g0.at[x], at_x(k)) for k in hops]
    second1 = [send(3, k, g1.at[y], g1.at[y], at_y(k)) for k in hops]
    up1 = [
        send(4, k, w_up.at[pl.ds(to_x(k) * side, side)], wb1.at[x], at_x(k)) for k in hops
    ]
    wb1[x] = w_up[pl.ds(x * side, side)]

    def pack_rows(s, carry):
        keys[pl.ds(pl.multiple_of(s * page, page), page), :] = spread[
            pl.ds(s * pitch, page), :
        ].astype(BF16)
        return carry

    lax.fori_loop(0, slots, pack_rows, 0, unroll=4)

    def owner_of(slot):
        return jnp.clip(owner_s[0, slot], 0, seqs - 1)

    row = lax.broadcasted_iota(jnp.int32, (seqs, 1), 0)
    length = jnp.zeros((seqs, 1), jnp.int32)
    for b in range(seqs):
        length = jnp.where(row == b, lengths[b], length)
    pages = lax.broadcasted_iota(jnp.int32, table.shape, 1)
    tokens = jnp.clip(length - page * pages, 0, page).astype(F32)
    relative = table[...] - me * slots
    lane8 = lax.broadcasted_iota(jnp.int32, (seqs, 128), 1)
    token = lax.rem(lane8, page).astype(F32)

    def fill_pair(i, owner):
        f0 = jnp.max(jnp.where(relative == 2 * i, tokens, 0.0), axis=1, keepdims=True)
        f1 = jnp.max(jnp.where(relative == 2 * i + 1, tokens, 0.0), axis=1, keepdims=True)
        fills[i] = jnp.where(lane8 < page, f0, f1) - token
        owner = jnp.where((lane8 == 2 * i) & (f0 > 0.0), row, owner)
        return jnp.where((lane8 == 2 * i + 1) & (f1 > 0.0), row, owner)

    owner = lax.fori_loop(
        0, slots // 2, fill_pair, jnp.zeros((seqs, 128), jnp.int32), unroll=2
    )
    owner_v[...] = jnp.broadcast_to(
        jnp.max(owner.astype(F32), axis=0, keepdims=True), owner.shape
    ).astype(jnp.int32)
    own_copy = pltpu.make_async_copy(owner_v, owner_s, own_sem)
    own_copy.start()

    for b in range(seqs):
        q_all[b, :, width:] = jnp.concatenate([q_rope[b], q_rope[b]], axis=-1)

    arrive(up1)
    up2 = [send(5, k, wb1.at[:, to_y(k)], wb2.at[:, y], at_y(k)) for k in hops]
    wb2[:, y] = wb1[:, y]
    own_copy.wait()
    arrive(second0)
    arrive(second1)

    eye = (
        lax.broadcasted_iota(jnp.int32, (half, half), 0)
        == lax.broadcasted_iota(jnp.int32, (half, half), 1)
    ).astype(BF16)
    columns0 = g0[...].reshape(width, half)
    columns1 = jnp.concatenate(
        [g1[:, i].reshape(side * cols, half) for i in range(side)], axis=0
    )
    for i, columns in enumerate((columns0, columns1)):
        rows = dot(eye, columns, NT).astype(BF16).reshape(seqs // 2, heads, width)
        q_all[i * (seqs // 2) : (i + 1) * (seqs // 2), :, :width] = rows

    for copy in lat_copies:
        copy.wait()

    def score_group(g, carry):
        picked = jnp.concatenate([q_all[owner_of(4 * g + j)] for j in range(4)], axis=0)
        tok = lat[pl.ds(g * 4, 4)].reshape(4 * page, width)
        rot = keys[pl.ds(pl.multiple_of(g * 4 * page, 4 * page), 4 * page), :]
        s = dot(picked[:, :width], tok, NT) + dot(picked[:, width:], rot, NT)
        for j in range(2):
            r, c = 2 * heads * j, 2 * page * j
            sc[2 * g + j] = jnp.where(
                low,
                s[r : r + heads, c : c + 2 * page],
                s[r + heads : r + 2 * heads, c : c + 2 * page],
            )
        return carry

    lax.fori_loop(0, slots // 4, score_group, 0)

    n_pairs = slots // 2
    for b in range(0, seqs, 2):

        def pair_max(i, carry):
            m0, m1 = carry
            s = sc[i]
            m0 = jnp.maximum(m0, jnp.where(fills[i, b : b + 1] > 0.0, s, NEG))
            m1 = jnp.maximum(m1, jnp.where(fills[i, b + 1 : b + 2] > 0.0, s, NEG))
            return m0, m1

        start = jnp.full((heads, 128), NEG, F32)
        m0, m1 = lax.fori_loop(0, n_pairs, pair_max, (start, start), unroll=4)
        for d, m in enumerate((m0, m1)):
            mrow[b + d] = jnp.broadcast_to(jnp.max(m, axis=1, keepdims=True), (heads, 128))

    head_lane = lax.broadcasted_iota(jnp.int32, (heads, 128), 1)
    head_row = lax.broadcasted_iota(jnp.int32, (heads, 128), 0)
    diag = head_lane == head_row

    def to_lanes(ref):
        return jnp.concatenate(
            [
                jnp.sum(jnp.where(diag, ref[b], 0.0), axis=0, keepdims=True)
                for b in range(seqs)
            ],
            axis=0,
        )

    mtile[...] = to_lanes(mrow)
    max1 = [send(6, k, mtile, mx.at[x], at_x(k)) for k in hops]

    factor = scale * math.log2(math.e)
    n_chunks = 4
    per = n_pairs // n_chunks
    acc[...] = jnp.zeros(acc.shape, F32)
    lrow[...] = jnp.zeros(lrow.shape, F32)
    for c in range(n_chunks):

        def weigh(i, carry):
            i = c * per + i
            top = jnp.where(low, mrow[owner_of(2 * i)], mrow[owner_of(2 * i + 1)])
            live = jnp.max(fills[i], axis=0, keepdims=True) > 0.0
            sc[i] = jnp.where(live, jnp.exp2((sc[i] - top) * factor), 0.0)
            return carry

        lax.fori_loop(0, per, weigh, 0, unroll=2)
        for b in range(seqs):

            def place(i, total):
                p = jnp.where(fills[c * per + i, b : b + 1] > 0.0, sc[c * per + i], 0.0)
                probs[
                    b * heads : (b + 1) * heads, pl.ds(pl.multiple_of(i * 128, 128), 128)
                ] = p.astype(BF16)
                return total + p

            lrow[b] = lax.fori_loop(0, per, place, lrow[b], unroll=4)
        n_tok = per * 2
        acc[...] += dot(
            probs[...], lat[c * n_tok : (c + 1) * n_tok].reshape(n_tok * page, width), NN
        )
        if c == 1:
            arrive(max1)
            top = mtile[...]
            for k in hops:
                top = jnp.maximum(top, mx[to_x(k)])
            mt2[...] = top
            max2 = [send(7, k, mt2, my.at[y], at_y(k)) for k in hops]

    arrive(max2)
    top = mt2[...]
    for k in hops:
        top = jnp.maximum(top, my[to_y(k)])

    tiles = hw // 128

    def every(ref, start, count):
        return jnp.concatenate(
            [ref[t, pl.ds(start, count, stride=side), :] for t in range(tiles)], axis=1
        ).astype(BF16)

    def put(ref, b, rows):
        for t in range(tiles):
            ref[t, b * side : (b + 1) * side, :] = rows[:, 128 * t : 128 * (t + 1)]

    for b in range(seqs):
        above = jnp.sum(
            jnp.where(diag, jnp.broadcast_to(top[b : b + 1], (heads, 128)), 0.0),
            axis=1,
            keepdims=True,
        )
        f = jnp.exp2((mrow[b] - above) * factor)
        lrow[b] = f * jnp.sum(lrow[b], axis=1, keepdims=True)
        rows = acc[b * heads : (b + 1) * heads, :] * f[:, :1]
        for t in range(tiles):
            stage[t, b * heads : (b + 1) * heads, :] = rows[
                :, hw + 128 * t : hw + 128 * (t + 1)
            ]
        sx[:, b] = rows[:, :hw].astype(BF16).reshape(side, side, hw)
    sum1 = [send(8, k, sx.at[to_x(k)], rx.at[x], at_x(k)) for k in hops]
    for b in range(seqs):
        for i in range(side):
            sy[i, b] = every(stage, b * heads + i, side)
    sum2 = [send(9, k, sy.at[to_y(k)], ry.at[y], at_y(k)) for k in hops]
    ltile[...] = to_lanes(lrow)
    tot1 = [send(10, k, ltile, lx.at[x], at_x(k)) for k in hops]

    arrive(sum1)
    for b in range(seqs):
        rows = sx[x, b].astype(F32)
        for k in hops:
            rows += rx[to_x(k), b].astype(F32)
        put(r0, b, rows)
    for i in range(side):
        s2y[i] = every(r0, i, seqs)
    fin1 = [send(11, k, s2y.at[to_y(k)], r2y.at[y], at_y(k)) for k in hops]
    arrive(sum2)
    for b in range(seqs):
        rows = sy[y, b].astype(F32)
        for k in hops:
            rows += ry[to_y(k), b].astype(F32)
        put(r1, b, rows)
    for i in range(side):
        s2x[i] = every(r1, i, seqs)
    fin2 = [send(12, k, s2x.at[to_x(k)], r2x.at[x], at_x(k)) for k in hops]
    arrive(tot1)
    total = ltile[...]
    for k in hops:
        total += lx[to_x(k)]
    lt2[...] = total
    tot2 = [send(13, k, lt2, ly.at[y], at_y(k)) for k in hops]

    arrive(fin1)
    att0 = s2y[y].astype(F32)
    for k in hops:
        att0 += r2y[to_y(k)].astype(F32)
    arrive(fin2)
    att1 = s2x[x].astype(F32)
    for k in hops:
        att1 += r2x[to_x(k)].astype(F32)
    arrive(tot2)
    total = lt2[...]
    for k in hops:
        total += ly[to_y(k)]
    total = jnp.sum(jnp.where(lane8 == me, total, 0.0), axis=1, keepdims=True)
    attention = (jnp.concatenate([att0, att1], axis=1) / total).astype(BF16)

    arrive(up2)
    value = dot(attention, wb2[...].reshape(width, wb2.shape[-1]), NN).astype(BF16)
    vals[x, y] = value
    val1 = [send(14, k, vals.at[x, y], vals.at[x, y], at_y(k)) for k in hops]
    wout_copy.wait()
    arrive(val1)
    val2 = [send(15, k, vals.at[x], vals.at[x], at_x(k)) for k in hops]
    arrive(val2)
    flat = jnp.concatenate(
        [vals[i, j] for i in range(side) for j in range(side)], axis=1
    )
    partial = dot(flat, wout[...], NT)
    width_out = partial.shape[1]
    part_send[:, :width_out] = partial
    swap = pltpu.make_async_remote_copy(
        src_ref=part_send,
        dst_ref=part_recv,
        send_sem=mp_sem.at[0],
        recv_sem=mp_sem.at[1],
        device_id={"mp": 1 - mp},
        device_id_type=pl.DeviceIdType.MESH,
    )
    swap.start()
    swap.wait()
    both = partial + part_recv[:, :width_out]
    n_out = out.shape[1]
    out[...] = jnp.where(mp == 0, both[:, :n_out], both[:, n_out:]).astype(BF16)
    for copy in started:
        copy.wait_send()


def local(
    latent_cache, rope_cache, q_nope, q_rope, w_uk, value_up_weight, w_out, page_table, lengths
):
    slots, page, width = latent_cache.shape
    seqs, heads, nope = q_nope.shape
    cols, vdim = value_up_weight.shape[1:]
    side = math.isqrt(lax.axis_size("seq"))
    scale = (nope + q_rope.shape[2]) ** (-0.5)
    n_out = w_out.shape[1] // lax.axis_size("mp")
    half = seqs * heads // 2
    hw = width // 2
    chunk = slots * page // 4
    pitch = page + 4
    vm = pltpu.VMEM
    anywhere = pl.BlockSpec(memory_space=pl.ANY)
    in_vmem = pl.BlockSpec(memory_space=pltpu.VMEM)
    scratch = [
        vm((slots, page, width), BF16),
        vm(rope_cache.shape, BF16),
        vm((w_out.shape[1], w_out.shape[0]), BF16),
        vm((slots * pitch + page, 128), F32),
        vm((slots * page, 128), BF16),
        vm((seqs, heads, width + 128), BF16),
        vm((side, side, cols, half), BF16),
        vm((side, side, cols, half), BF16),
        vm((side, side, cols, vdim), BF16),
        vm((side, side, cols, vdim), BF16),
        vm((slots // 2, seqs, 128), F32),
        vm((seqs, 128), jnp.int32),
        pltpu.SMEM((seqs, 128), jnp.int32),
        vm((slots // 2, heads, 128), F32),
        vm((seqs, heads, 128), F32),
        vm((seqs, heads, 128), F32),
        vm((seqs * heads, chunk), BF16),
        vm((seqs * heads, width), F32),
        vm((seqs, 128), F32),
        vm((side, seqs, 128), F32),
        vm((seqs, 128), F32),
        vm((side, seqs, 128), F32),
        vm((seqs, 128), F32),
        vm((side, seqs, 128), F32),
        vm((seqs, 128), F32),
        vm((side, seqs, 128), F32),
        vm((side, seqs, side, hw), BF16),
        vm((side, seqs, side, hw), BF16),
        vm((side, seqs, side, hw), BF16),
        vm((side, seqs, side, hw), BF16),
        vm((hw // 128, seqs * heads + side, 128), F32),
        vm((hw // 128, seqs * side + side, 128), F32),
        vm((hw // 128, seqs * side + side, 128), F32),
        vm((side, seqs, hw), BF16),
        vm((side, seqs, hw), BF16),
        vm((side, seqs, hw), BF16),
        vm((side, seqs, hw), BF16),
        vm((side, side, seqs, vdim), BF16),
        vm((seqs, 128), F32),
        vm((seqs, 128), F32),
        pltpu.SemaphoreType.DMA((6,)),
        pltpu.SemaphoreType.DMA,
        pltpu.SemaphoreType.DMA((16, side)),
        pltpu.SemaphoreType.DMA((16, side)),
        pltpu.SemaphoreType.DMA((2,)),
    ]
    return pl.pallas_call(
        functools.partial(kernel, side, scale),
        out_shape=jax.ShapeDtypeStruct((seqs, n_out), BF16),
        in_specs=[in_vmem] * 5
        + [pl.BlockSpec(memory_space=pltpu.SMEM)]
        + [anywhere] * 3,
        out_specs=in_vmem,
        scratch_shapes=scratch,
        compiler_params=pltpu.CompilerParams(
            collective_id=0, has_side_effects=True, vmem_limit_bytes=60 * 1024 * 1024
        ),
        name="decode",
    )(
        q_nope,
        q_rope,
        jnp.swapaxes(w_uk, 1, 2),
        value_up_weight,
        page_table,
        lengths,
        latent_cache,
        rope_cache,
        jnp.swapaxes(w_out, 0, 1),
    )


def solution(mesh):
    return jax.shard_map(
        local,
        mesh=mesh,
        in_specs=(
            P(GROUPS_SEQ, None, None),
            P(GROUPS_SEQ, None),
            P("groups", "mp", None),
            P("groups", "mp", None),
            P("mp", None, "seq"),
            P("mp", "seq", None),
            P("mp", "seq"),
            P("groups", None),
            P("groups"),
        ),
        out_specs=P("groups", ("seq", "mp")),
        check_vma=False,
    )
```

```python
import functools
import math

import jax
import jax.numpy as jnp
from jax import lax
from jax.experimental import pallas as pl
from jax.experimental.pallas import tpu as pltpu
from jax.sharding import PartitionSpec as P

GROUPS_SEQ = ("groups", "seq")
NEG = -1e30
F32 = jnp.float32
BF16 = jnp.bfloat16
NT = (((1,), (1,)), ((), ()))
NN = (((1,), (0,)), ((), ()))


def dot(a, b, dims):
    return lax.dot_general(a, b, dims, preferred_element_type=F32)


def kernel(
    side,
    scale,
    q_nope,
    q_rope,
    w_uk,
    w_up,
    table,
    lengths,
    latent_hbm,
    rope_hbm,
    w_out_hbm,
    out,
    lat,
    rope,
    wout,
    spread,
    keys,
    q_all,
    g0,
    g1,
    wb1,
    wb2,
    fills,
    owner_v,
    owner_s,
    sc,
    mrow,
    lrow,
    mrun,
    probs,
    acc,
    maskt,
    maskl,
    mtile,
    mx,
    mt2,
    my,
    my2,
    ltile,
    lx,
    lt2,
    ly,
    sx,
    sy,
    rx,
    ry,
    stage,
    r0,
    r1,
    s2y,
    s2x,
    r2y,
    r2x,
    vals,
    part_send,
    part_recv,
    load_sem,
    own_sem,
    send_sem,
    recv_sem,
    mp_sem,
):
    seqs, heads, nope = q_nope.shape
    slots, page, width = lat.shape
    half = seqs * heads // 2
    hw = width // 2
    me = lax.axis_index("seq")
    mp = lax.axis_index("mp")
    x, y = lax.div(me, side), lax.rem(me, side)
    hops = sorted(range(1, side), key=lambda k: -min(k, side - k))

    def to_x(k):
        return lax.rem(x + k, side)

    def to_y(k):
        return lax.rem(y + k, side)

    def at_x(k):
        return {"seq": to_x(k) * side + y}

    def at_y(k):
        return {"seq": x * side + to_y(k)}

    loads = []
    n_cut = 4
    cut = slots // n_cut

    def load(src, dst):
        copy = pltpu.make_async_copy(src, dst, load_sem.at[len(loads)])
        copy.start()
        loads.append(copy)

    load(rope_hbm, rope)
    for i in range(n_cut):
        load(latent_hbm.at[pl.ds(i * cut, cut)], lat.at[pl.ds(i * cut, cut)])
    load(w_out_hbm, wout)

    barrier = pltpu.get_barrier_semaphore()
    for k in hops:
        pl.semaphore_signal(barrier, inc=1, device_id=at_x(k), device_id_type=pl.DeviceIdType.MESH)
        pl.semaphore_signal(barrier, inc=1, device_id=at_y(k), device_id_type=pl.DeviceIdType.MESH)
    pl.semaphore_signal(
        barrier, inc=1, device_id={"mp": 1 - mp}, device_id_type=pl.DeviceIdType.MESH
    )

    started = []

    def send(phase, k, src, dst, device):
        copy = pltpu.make_async_remote_copy(
            src_ref=src,
            dst_ref=dst,
            send_sem=send_sem.at[phase, k],
            recv_sem=recv_sem.at[phase, k],
            device_id=device,
            device_id_type=pl.DeviceIdType.MESH,
        )
        copy.start()
        started.append(copy)
        return copy

    def arrive(copies):
        for copy in copies:
            copy.wait_recv()

    cols = w_uk.shape[1]
    wide = dot(
        w_uk[...].reshape(heads * cols, nope), q_nope[...].reshape(seqs * heads, nope), NT
    ).reshape(heads, cols, seqs * heads)
    row_head = lax.broadcasted_iota(jnp.int32, wide.shape, 0)
    col_head = lax.rem(lax.broadcasted_iota(jnp.int32, wide.shape, 2), heads)
    q_part = jnp.sum(jnp.where(row_head == col_head, wide, 0.0), axis=0).astype(BF16)
    g0[x, y] = q_part[:, :half]
    g1[y, x] = q_part[:, half:]

    pl.semaphore_wait(barrier, 2 * (side - 1) + 1)

    first0 = [send(0, k, g0.at[x, y], g0.at[x, y], at_y(k)) for k in hops]
    first1 = [send(1, k, g1.at[y, x], g1.at[y, x], at_x(k)) for k in hops]

    lane = lax.broadcasted_iota(jnp.int32, (1, 128), 1)
    low = lane < page
    pitch = spread.shape[0] // slots
    rope_copy, lat_copies, wout_copy = loads[0], loads[1:-1], loads[-1]
    rope_copy.wait()

    def spread_pair(c, carry):
        z = rope[:, pl.ds(pl.multiple_of(c * 128, 128), 128)].astype(F32)
        spread[pl.ds(2 * c, slots, stride=pitch), :] = jnp.where(low, z, 0.0)
        spread[pl.ds(2 * c + 1, slots, stride=pitch), :] = jnp.where(low, 0.0, z)
        return carry

    lax.fori_loop(0, rope.shape[1] // 128, spread_pair, 0)

    def owner_of(slot):
        return jnp.clip(owner_s[0, slot], 0, seqs - 1)

    row = lax.broadcasted_iota(jnp.int32, (seqs, 1), 0)
    length = jnp.zeros((seqs, 1), jnp.int32)
    for b in range(seqs):
        length = jnp.where(row == b, lengths[b], length)
    pages = lax.broadcasted_iota(jnp.int32, table.shape, 1)
    tokens = jnp.clip(length - page * pages, 0, page).astype(F32)
    relative = table[...] - me * slots
    lane8 = lax.broadcasted_iota(jnp.int32, (seqs, 128), 1)
    token = lax.rem(lane8, page).astype(F32)

    def fill_pair(i, owner):
        f0 = jnp.max(jnp.where(relative == 2 * i, tokens, 0.0), axis=1, keepdims=True)
        f1 = jnp.max(jnp.where(relative == 2 * i + 1, tokens, 0.0), axis=1, keepdims=True)
        fills[i] = jnp.where(lane8 < page, f0, f1) - token
        owner = jnp.where((lane8 == 2 * i) & (f0 > 0.0), row, owner)
        return jnp.where((lane8 == 2 * i + 1) & (f1 > 0.0), row, owner)

    owner = lax.fori_loop(
        0, slots // 2, fill_pair, jnp.zeros((seqs, 128), jnp.int32), unroll=8
    )
    owner_v[...] = jnp.broadcast_to(
        jnp.max(owner.astype(F32), axis=0, keepdims=True), owner.shape
    ).astype(jnp.int32)
    own_copy = pltpu.make_async_copy(owner_v, owner_s, own_sem)
    own_copy.start()

    arrive(first0)
    arrive(first1)
    second0 = [send(2, k, g0.at[x], g0.at[x], at_x(k)) for k in hops]
    second1 = [send(3, k, g1.at[y], g1.at[y], at_y(k)) for k in hops]
    def pack_rows(s, carry):
        keys[pl.ds(pl.multiple_of(s * page, page), page), :] = spread[
            pl.ds(s * pitch, page), :
        ].astype(BF16)
        return carry

    lax.fori_loop(0, slots, pack_rows, 0, unroll=4)

    def mask_pair(i, carry):
        live = jnp.where(fills[i] > 0.0, 1.0, 0.0)
        maskl[i] = live.astype(BF16)
        for b in range(seqs):
            maskt[i, b] = jnp.broadcast_to(live[b : b + 1], (16, 128)).astype(BF16)
        return carry

    lax.fori_loop(0, slots // 2, mask_pair, 0, unroll=4)

    for b in range(seqs):
        q_all[b, :, width:] = jnp.concatenate([q_rope[b], q_rope[b]], axis=-1)

    own_copy.wait()
    arrive(second0)
    arrive(second1)

    up1 = [
        send(4, k, w_up.at[pl.ds(to_x(k) * side, side)], wb1.at[x], at_x(k)) for k in hops
    ]
    wb1[x] = w_up[pl.ds(x * side, side)]

    eye = (
        lax.broadcasted_iota(jnp.int32, (half, half), 0)
        == lax.broadcasted_iota(jnp.int32, (half, half), 1)
    ).astype(BF16)
    columns0 = g0[...].reshape(width, half)
    columns1 = jnp.concatenate(
        [g1[:, i].reshape(side * cols, half) for i in range(side)], axis=0
    )
    for i, columns in enumerate((columns0, columns1)):
        rows = dot(eye, columns, NT).astype(BF16).reshape(seqs // 2, heads, width)
        q_all[i * (seqs // 2) : (i + 1) * (seqs // 2), :, :width] = rows

    for copy in lat_copies:
        copy.wait()

    def score_group(g, carry):
        picked = jnp.concatenate([q_all[owner_of(4 * g + j)] for j in range(4)], axis=0)
        tok = lat[pl.ds(g * 4, 4)].reshape(4 * page, width)
        rot = keys[pl.ds(pl.multiple_of(g * 4 * page, 4 * page), 4 * page), :]
        s = dot(picked[:, :width], tok, NT) + dot(picked[:, width:], rot, NT)
        blocks = []
        for j in range(2):
            r, c = 2 * heads * j, 2 * page * j
            block = jnp.where(
                low,
                s[r : r + heads, c : c + 2 * page],
                s[r + heads : r + 2 * heads, c : c + 2 * page],
            )
            sc[2 * g + j] = block
            blocks.append(block)
        for b in range(seqs):
            m = mrun[b]
            for j in range(2):
                m = jnp.maximum(m, jnp.where(fills[2 * g + j, b : b + 1] > 0.0, blocks[j], NEG))
            mrun[b] = m
        return carry

    mrun[...] = jnp.full(mrun.shape, NEG, F32)
    lax.fori_loop(0, slots // 4, score_group, 0, unroll=8)
    for b in range(seqs):
        mrow[b] = jnp.broadcast_to(jnp.max(mrun[b], axis=1, keepdims=True), (heads, 128))

    head_lane = lax.broadcasted_iota(jnp.int32, (heads, 128), 1)
    head_row = lax.broadcasted_iota(jnp.int32, (heads, 128), 0)
    diag = head_lane == head_row

    def to_lanes(ref):
        return jnp.concatenate(
            [
                jnp.sum(jnp.where(diag, ref[b], 0.0), axis=0, keepdims=True)
                for b in range(seqs)
            ],
            axis=0,
        )

    mtile[...] = to_lanes(mrow)
    max1 = [send(6, k, mtile, mx.at[x], at_x(k)) for k in hops]
    max1y = [send(7, k, mtile, my.at[y], at_y(k)) for k in hops]
    arrive(up1)
    up2 = [send(5, k, wb1.at[:, to_y(k)], wb2.at[:, y], at_y(k)) for k in hops]
    wb2[:, y] = wb1[:, y]

    factor = scale * math.log2(math.e)
    n_pairs = slots // 2
    n_chunks = 4
    per = n_pairs // n_chunks
    n_tok = per * 2
    lsum = jnp.zeros((heads, seqs), F32)
    for c in range(n_chunks):
        for j in range(per):
            i = c * per + j
            top = jnp.where(low, mrow[owner_of(2 * i)], mrow[owner_of(2 * i + 1)])
            live = jnp.max(fills[i], axis=0, keepdims=True) > 0.0
            p = jnp.where(live, jnp.exp2((sc[i] - top) * factor), 0.0).astype(BF16)
            p16 = p.reshape(heads // 16, 16, 128)
            for b in range(seqs):
                probs[b * heads : (b + 1) * heads, j * 128 : (j + 1) * 128] = (
                    p16 * maskt[i, b][None]
                ).reshape(heads, 128)
            lsum += dot(p, maskl[i], NT)
        part = dot(
            probs[...], lat[c * n_tok : (c + 1) * n_tok].reshape(n_tok * page, width), NN
        )
        acc[...] = part if c == 0 else acc[...] + part
        if c == 2:
            arrive(max1)
            top_x = mtile[...]
            for k in hops:
                top_x = jnp.maximum(top_x, mx[to_x(k)])
            mt2[...] = top_x
            max2 = [send(16, k, mt2, my2.at[y], at_y(k)) for k in hops]

    arrive(max1y)
    top_x = mt2[...]
    top_y = mtile[...]
    for k in hops:
        top_y = jnp.maximum(top_y, my[to_y(k)])

    tiles = hw // 128

    def every(ref, start, count):
        return jnp.concatenate(
            [ref[t, pl.ds(start, count, stride=side), :] for t in range(tiles)], axis=1
        ).astype(BF16)

    def put(ref, b, rows):
        for t in range(tiles):
            ref[t, b * side : (b + 1) * side, :] = rows[:, 128 * t : 128 * (t + 1)]

    def column(tile, b):
        return jnp.sum(
            jnp.where(diag, jnp.broadcast_to(tile[b : b + 1], (heads, 128)), 0.0),
            axis=1,
            keepdims=True,
        )

    for b in range(seqs):
        local_top = mrow[b]
        f0 = jnp.exp2((local_top - column(top_x, b)) * factor)
        f1 = jnp.exp2((local_top - column(top_y, b)) * factor)
        lrow[b] = f0 * lsum[:, b : b + 1]
        rows = acc[b * heads : (b + 1) * heads, :]
        sx[:, b] = (rows[:, :hw] * f0[:, :1]).astype(BF16).reshape(side, side, hw)
        for t in range(tiles):
            stage[t, b * heads : (b + 1) * heads, :] = (
                rows[:, hw + 128 * t : hw + 128 * (t + 1)] * f1
            )
    sum1 = [send(8, k, sx.at[to_x(k)], rx.at[x], at_x(k)) for k in hops]
    for b in range(seqs):
        for i in range(side):
            sy[i, b] = every(stage, b * heads + i, side)
    sum2 = [send(9, k, sy.at[to_y(k)], ry.at[y], at_y(k)) for k in hops]
    ltile[...] = to_lanes(lrow)
    tot1 = [send(10, k, ltile, lx.at[x], at_x(k)) for k in hops]

    arrive(max2)
    top = top_x
    for k in hops:
        top = jnp.maximum(top, my2[to_y(k)])
    shrink_x = jnp.exp2((top_x - top) * factor)
    shrink_y = jnp.exp2((top_y - top) * factor)
    row8 = lax.broadcasted_iota(jnp.int32, (side, 128), 0)
    lane_of = lax.broadcasted_iota(jnp.int32, (side, 128), 1)

    def pick(tile, b, which):
        return jnp.sum(
            jnp.where(lane_of == which, jnp.broadcast_to(tile[b : b + 1], (side, 128)), 0.0),
            axis=1,
            keepdims=True,
        )

    arrive(sum1)
    for b in range(seqs):
        rows = sx[x, b].astype(F32)
        for k in hops:
            rows += rx[to_x(k), b].astype(F32)
        put(r0, b, rows * pick(shrink_x, b, x * side + row8))
    for i in range(side):
        s2y[i] = every(r0, i, seqs)
    fin1 = [send(11, k, s2y.at[to_y(k)], r2y.at[y], at_y(k)) for k in hops]
    arrive(sum2)
    for b in range(seqs):
        rows = sy[y, b].astype(F32)
        for k in hops:
            rows += ry[to_y(k), b].astype(F32)
        put(r1, b, rows * pick(shrink_y, b, row8 * side + y))
    for i in range(side):
        s2x[i] = every(r1, i, seqs)
    fin2 = [send(12, k, s2x.at[to_x(k)], r2x.at[x], at_x(k)) for k in hops]
    arrive(tot1)
    total = ltile[...]
    for k in hops:
        total += lx[to_x(k)]
    lt2[...] = total * shrink_x
    tot2 = [send(13, k, lt2, ly.at[y], at_y(k)) for k in hops]

    arrive(fin1)
    att0 = s2y[y].astype(F32)
    for k in hops:
        att0 += r2y[to_y(k)].astype(F32)
    arrive(fin2)
    att1 = s2x[x].astype(F32)
    for k in hops:
        att1 += r2x[to_x(k)].astype(F32)
    arrive(tot2)
    total = lt2[...]
    for k in hops:
        total += ly[to_y(k)]
    total = jnp.sum(jnp.where(lane8 == me, total, 0.0), axis=1, keepdims=True)
    attention = (jnp.concatenate([att0, att1], axis=1) / total).astype(BF16)

    arrive(up2)
    value = dot(attention, wb2[...].reshape(width, wb2.shape[-1]), NN).astype(BF16)
    vals[x, y] = value
    val1 = [send(14, k, vals.at[x, y], vals.at[x, y], at_y(k)) for k in hops]
    wout_copy.wait()
    arrive(val1)
    val2 = [send(15, k, vals.at[x], vals.at[x], at_x(k)) for k in hops]
    arrive(val2)
    flat = jnp.concatenate(
        [vals[i, j] for i in range(side) for j in range(side)], axis=1
    )
    partial = dot(flat, wout[...], NT)
    width_out = partial.shape[1]
    part_send[:, :width_out] = partial
    swap = pltpu.make_async_remote_copy(
        src_ref=part_send,
        dst_ref=part_recv,
        send_sem=mp_sem.at[0],
        recv_sem=mp_sem.at[1],
        device_id={"mp": 1 - mp},
        device_id_type=pl.DeviceIdType.MESH,
    )
    swap.start()
    swap.wait()
    both = partial + part_recv[:, :width_out]
    n_out = out.shape[1]
    out[...] = jnp.where(mp == 0, both[:, :n_out], both[:, n_out:]).astype(BF16)
    for copy in started:
        copy.wait_send()


def local(
    latent_cache, rope_cache, q_nope, q_rope, w_uk, value_up_weight, w_out, page_table, lengths
):
    slots, page, width = latent_cache.shape
    seqs, heads, nope = q_nope.shape
    cols, vdim = value_up_weight.shape[1:]
    side = math.isqrt(lax.axis_size("seq"))
    scale = (nope + q_rope.shape[2]) ** (-0.5)
    n_out = w_out.shape[1] // lax.axis_size("mp")
    half = seqs * heads // 2
    hw = width // 2
    chunk = slots * page // 4
    pitch = page + 4
    vm = pltpu.VMEM
    anywhere = pl.BlockSpec(memory_space=pl.ANY)
    in_vmem = pl.BlockSpec(memory_space=pltpu.VMEM)
    scratch = [
        vm((slots, page, width), BF16),
        vm(rope_cache.shape, BF16),
        vm((w_out.shape[1], w_out.shape[0]), BF16),
        vm((slots * pitch + page, 128), F32),
        vm((slots * page, 128), BF16),
        vm((seqs, heads, width + 128), BF16),
        vm((side, side, cols, half), BF16),
        vm((side, side, cols, half), BF16),
        vm((side, side, cols, vdim), BF16),
        vm((side, side, cols, vdim), BF16),
        vm((slots // 2, seqs, 128), F32),
        vm((seqs, 128), jnp.int32),
        pltpu.SMEM((seqs, 128), jnp.int32),
        vm((slots // 2, heads, 128), F32),
        vm((seqs, heads, 128), F32),
        vm((seqs, heads, 128), F32),
        vm((seqs, heads, 128), F32),
        vm((seqs * heads, chunk), BF16),
        vm((seqs * heads, width), F32),
        vm((slots // 2, seqs, 16, 128), BF16),
        vm((slots // 2, seqs, 128), BF16),
        vm((seqs, 128), F32),
        vm((side, seqs, 128), F32),
        vm((seqs, 128), F32),
        vm((side, seqs, 128), F32),
        vm((side, seqs, 128), F32),
        vm((seqs, 128), F32),
        vm((side, seqs, 128), F32),
        vm((seqs, 128), F32),
        vm((side, seqs, 128), F32),
        vm((side, seqs, side, hw), BF16),
        vm((side, seqs, side, hw), BF16),
        vm((side, seqs, side, hw), BF16),
        vm((side, seqs, side, hw), BF16),
        vm((hw // 128, seqs * heads + side, 128), F32),
        vm((hw // 128, seqs * side + side, 128), F32),
        vm((hw // 128, seqs * side + side, 128), F32),
        vm((side, seqs, hw), BF16),
        vm((side, seqs, hw), BF16),
        vm((side, seqs, hw), BF16),
        vm((side, seqs, hw), BF16),
        vm((side, side, seqs, vdim), BF16),
        vm((seqs, 128), F32),
        vm((seqs, 128), F32),
        pltpu.SemaphoreType.DMA((6,)),
        pltpu.SemaphoreType.DMA,
        pltpu.SemaphoreType.DMA((17, side)),
        pltpu.SemaphoreType.DMA((17, side)),
        pltpu.SemaphoreType.DMA((2,)),
    ]
    return pl.pallas_call(
        functools.partial(kernel, side, scale),
        out_shape=jax.ShapeDtypeStruct((seqs, n_out), BF16),
        in_specs=[in_vmem] * 5
        + [pl.BlockSpec(memory_space=pltpu.SMEM)]
        + [anywhere] * 3,
        out_specs=in_vmem,
        scratch_shapes=scratch,
        compiler_params=pltpu.CompilerParams(
            collective_id=0, has_side_effects=True, vmem_limit_bytes=60 * 1024 * 1024
        ),
        name="decode",
    )(
        q_nope,
        q_rope,
        jnp.swapaxes(w_uk, 1, 2),
        value_up_weight,
        page_table,
        lengths,
        latent_cache,
        rope_cache,
        jnp.swapaxes(w_out, 0, 1),
    )


def solution(mesh):
    return jax.shard_map(
        local,
        mesh=mesh,
        in_specs=(
            P(GROUPS_SEQ, None, None),
            P(GROUPS_SEQ, None),
            P("groups", "mp", None),
            P("groups", "mp", None),
            P("mp", None, "seq"),
            P("mp", "seq", None),
            P("mp", "seq"),
            P("groups", None),
            P("groups"),
        ),
        out_specs=P("groups", ("seq", "mp")),
        check_vma=False,
    )
```

```python
import functools
import math

import jax
import jax.numpy as jnp
from jax import lax
from jax.experimental import pallas as pl
from jax.experimental.pallas import tpu as pltpu
from jax.sharding import PartitionSpec as P

GROUPS_SEQ = ("groups", "seq")
NEG = -1e30
F32 = jnp.float32
BF16 = jnp.bfloat16
NT = (((1,), (1,)), ((), ()))
NN = (((1,), (0,)), ((), ()))


def dot(a, b, dims):
    return lax.dot_general(a, b, dims, preferred_element_type=F32)


def kernel(
    side,
    scale,
    q_nope_hbm,
    q_rope_hbm,
    w_uk_hbm,
    w_up_hbm,
    table_hbm,
    lengths_hbm,
    latent_hbm,
    rope_hbm,
    w_out_hbm,
    out,
    q_nope,
    q_rope,
    w_uk,
    w_up,
    table,
    lengths,
    lat,
    rope,
    wout,
    spread,
    keys,
    q_all,
    g0,
    g1,
    wb1,
    wb2,
    fills,
    owner_v,
    owner_s,
    sc,
    mrow,
    lrow,
    mrun,
    probs,
    acc,
    maskt,
    maskl,
    mtile,
    mx,
    mt2,
    my,
    my2,
    ltile,
    lx,
    lt2,
    ly,
    sx,
    sy,
    rx,
    ry,
    stage,
    r0,
    r1,
    s2y,
    s2x,
    r2y,
    r2x,
    vals,
    part_send,
    part_recv,
    load_sem,
    own_sem,
    send_sem,
    recv_sem,
    mp_sem,
):
    seqs, heads, nope = q_nope.shape
    slots, page, width = lat.shape
    half = seqs * heads // 2
    hw = width // 2
    me = lax.axis_index("seq")
    mp = lax.axis_index("mp")
    x, y = lax.div(me, side), lax.rem(me, side)
    hops = sorted(range(1, side), key=lambda k: -min(k, side - k))

    def to_x(k):
        return lax.rem(x + k, side)

    def to_y(k):
        return lax.rem(y + k, side)

    def at_x(k):
        return {"seq": to_x(k) * side + y}

    def at_y(k):
        return {"seq": x * side + to_y(k)}

    barrier = pltpu.get_barrier_semaphore()
    for k in hops:
        pl.semaphore_signal(barrier, inc=1, device_id=at_x(k), device_id_type=pl.DeviceIdType.MESH)
        pl.semaphore_signal(barrier, inc=1, device_id=at_y(k), device_id_type=pl.DeviceIdType.MESH)
    pl.semaphore_signal(
        barrier, inc=1, device_id={"mp": 1 - mp}, device_id_type=pl.DeviceIdType.MESH
    )

    loads = []
    n_cut = 4
    cut = slots // n_cut

    def load(src, dst):
        copy = pltpu.make_async_copy(src, dst, load_sem.at[len(loads)])
        copy.start()
        loads.append(copy)
        return copy

    query_copies = [load(q_nope_hbm, q_nope), load(w_uk_hbm, w_uk)]
    rope_copy = load(rope_hbm, rope)
    table_copies = [load(table_hbm, table), load(lengths_hbm, lengths)]
    side_copies = [load(q_rope_hbm, q_rope), load(w_up_hbm, w_up)]
    lat_copies = [
        load(latent_hbm.at[pl.ds(i * cut, cut)], lat.at[pl.ds(i * cut, cut)])
        for i in range(n_cut)
    ]
    wout_copy = load(w_out_hbm, wout)

    started = []

    def send(phase, k, src, dst, device):
        copy = pltpu.make_async_remote_copy(
            src_ref=src,
            dst_ref=dst,
            send_sem=send_sem.at[phase, k],
            recv_sem=recv_sem.at[phase, k],
            device_id=device,
            device_id_type=pl.DeviceIdType.MESH,
        )
        copy.start()
        started.append(copy)
        return copy

    def arrive(copies):
        for copy in copies:
            copy.wait_recv()

    for copy in query_copies:
        copy.wait()

    cols = w_uk.shape[1]
    wide = dot(
        w_uk[...].reshape(heads * cols, nope), q_nope[...].reshape(seqs * heads, nope), NT
    ).reshape(heads, cols, seqs * heads)
    row_head = lax.broadcasted_iota(jnp.int32, wide.shape, 0)
    col_head = lax.rem(lax.broadcasted_iota(jnp.int32, wide.shape, 2), heads)
    q_part = jnp.sum(jnp.where(row_head == col_head, wide, 0.0), axis=0).astype(BF16)
    g0[x, y] = q_part[:, :half]
    g1[y, x] = q_part[:, half:]

    pl.semaphore_wait(barrier, 2 * (side - 1) + 1)

    near = hops[::-1]
    first0 = {k: send(0, k, g0.at[x, y], g0.at[x, y], at_y(k)) for k in hops}
    first1 = {k: send(1, k, g1.at[y, x], g1.at[y, x], at_x(k)) for k in hops}

    def forward(phase, k, piece, device):
        return pltpu.make_async_remote_copy(
            src_ref=piece,
            dst_ref=piece,
            send_sem=send_sem.at[phase, k],
            recv_sem=recv_sem.at[phase, k],
            device_id=device,
            device_id_type=pl.DeviceIdType.MESH,
        )

    def pass_on(row, col):
        for k in hops:
            forward(2, k, g0.at[x, row], at_x(k)).start()
            forward(3, k, g1.at[y, col], at_y(k)).start()

    second0 = [forward(2, k, g0.at[x], at_x(k)) for k in hops]
    second1 = [forward(3, k, g1.at[y], at_y(k)) for k in hops]
    started.extend(second0 + second1)
    pass_on(y, x)

    lane = lax.broadcasted_iota(jnp.int32, (1, 128), 1)
    low = lane < page
    pitch = spread.shape[0] // slots
    rope_copy.wait()

    def spread_pair(c, carry):
        z = rope[:, pl.ds(pl.multiple_of(c * 128, 128), 128)].astype(F32)
        spread[pl.ds(2 * c, slots, stride=pitch), :] = jnp.where(low, z, 0.0)
        spread[pl.ds(2 * c + 1, slots, stride=pitch), :] = jnp.where(low, 0.0, z)
        return carry

    lax.fori_loop(0, rope.shape[1] // 128, spread_pair, 0)

    def owner_of(slot):
        return jnp.clip(owner_s[0, slot], 0, seqs - 1)

    for copy in table_copies:
        copy.wait()

    row = lax.broadcasted_iota(jnp.int32, (seqs, 1), 0)
    length = jnp.zeros((seqs, 1), jnp.int32)
    for b in range(seqs):
        length = jnp.where(row == b, lengths[b], length)
    pages = lax.broadcasted_iota(jnp.int32, table.shape, 1)
    tokens = jnp.clip(length - page * pages, 0, page).astype(F32)
    relative = table[...] - me * slots
    lane8 = lax.broadcasted_iota(jnp.int32, (seqs, 128), 1)
    token = lax.rem(lane8, page).astype(F32)

    def fill_pair(i, owner):
        f0 = jnp.max(jnp.where(relative == 2 * i, tokens, 0.0), axis=1, keepdims=True)
        f1 = jnp.max(jnp.where(relative == 2 * i + 1, tokens, 0.0), axis=1, keepdims=True)
        fills[i] = jnp.where(lane8 < page, f0, f1) - token
        owner = jnp.where((lane8 == 2 * i) & (f0 > 0.0), row, owner)
        return jnp.where((lane8 == 2 * i + 1) & (f1 > 0.0), row, owner)

    owner = lax.fori_loop(
        0, slots // 2, fill_pair, jnp.zeros((seqs, 128), jnp.int32), unroll=8
    )
    owner_v[...] = jnp.broadcast_to(
        jnp.max(owner.astype(F32), axis=0, keepdims=True), owner.shape
    ).astype(jnp.int32)
    own_copy = pltpu.make_async_copy(owner_v, owner_s, own_sem)
    own_copy.start()

    for k in near:
        first0[k].wait_recv()
        first1[k].wait_recv()
        pass_on(to_y(side - k), to_x(side - k))
    def pack_rows(s, carry):
        keys[pl.ds(pl.multiple_of(s * page, page), page), :] = spread[
            pl.ds(s * pitch, page), :
        ].astype(BF16)
        return carry

    lax.fori_loop(0, slots, pack_rows, 0, unroll=4)

    def mask_pair(i, carry):
        live = jnp.where(fills[i] > 0.0, 1.0, 0.0)
        maskl[i] = live.astype(BF16)
        for b in range(seqs):
            maskt[i, b] = jnp.broadcast_to(live[b : b + 1], (16, 128)).astype(BF16)
        return carry

    lax.fori_loop(0, slots // 2, mask_pair, 0, unroll=4)

    for copy in side_copies:
        copy.wait()
    for b in range(seqs):
        q_all[b, :, width:] = jnp.concatenate([q_rope[b], q_rope[b]], axis=-1)

    own_copy.wait()
    arrive(second0)
    arrive(second1)

    up1 = [
        send(4, k, w_up.at[pl.ds(to_x(k) * side, side)], wb1.at[x], at_x(k)) for k in hops
    ]
    wb1[x] = w_up[pl.ds(x * side, side)]

    eye = (
        lax.broadcasted_iota(jnp.int32, (half, half), 0)
        == lax.broadcasted_iota(jnp.int32, (half, half), 1)
    ).astype(BF16)
    columns0 = g0[...].reshape(width, half)
    columns1 = jnp.concatenate(
        [g1[:, i].reshape(side * cols, half) for i in range(side)], axis=0
    )
    for i, columns in enumerate((columns0, columns1)):
        rows = dot(eye, columns, NT).astype(BF16).reshape(seqs // 2, heads, width)
        q_all[i * (seqs // 2) : (i + 1) * (seqs // 2), :, :width] = rows

    for copy in lat_copies:
        copy.wait()

    def score_group(g, carry):
        picked = jnp.concatenate([q_all[owner_of(4 * g + j)] for j in range(4)], axis=0)
        tok = lat[pl.ds(g * 4, 4)].reshape(4 * page, width)
        rot = keys[pl.ds(pl.multiple_of(g * 4 * page, 4 * page), 4 * page), :]
        s = dot(picked[:, :width], tok, NT) + dot(picked[:, width:], rot, NT)
        blocks = []
        for j in range(2):
            r, c = 2 * heads * j, 2 * page * j
            block = jnp.where(
                low,
                s[r : r + heads, c : c + 2 * page],
                s[r + heads : r + 2 * heads, c : c + 2 * page],
            )
            sc[2 * g + j] = block
            blocks.append(block)
        for b in range(seqs):
            m = mrun[b]
            for j in range(2):
                m = jnp.maximum(m, jnp.where(fills[2 * g + j, b : b + 1] > 0.0, blocks[j], NEG))
            mrun[b] = m
        return carry

    mrun[...] = jnp.full(mrun.shape, NEG, F32)
    lax.fori_loop(0, slots // 4, score_group, 0, unroll=8)
    for b in range(seqs):
        mrow[b] = jnp.broadcast_to(jnp.max(mrun[b], axis=1, keepdims=True), (heads, 128))

    head_lane = lax.broadcasted_iota(jnp.int32, (heads, 128), 1)
    head_row = lax.broadcasted_iota(jnp.int32, (heads, 128), 0)
    diag = head_lane == head_row

    def to_lanes(ref):
        return jnp.concatenate(
            [
                jnp.sum(jnp.where(diag, ref[b], 0.0), axis=0, keepdims=True)
                for b in range(seqs)
            ],
            axis=0,
        )

    mtile[...] = to_lanes(mrow)
    max1 = [send(6, k, mtile, mx.at[x], at_x(k)) for k in hops]
    max1y = [send(7, k, mtile, my.at[y], at_y(k)) for k in hops]
    arrive(up1)
    up2 = [send(5, k, wb1.at[:, to_y(k)], wb2.at[:, y], at_y(k)) for k in hops]
    wb2[:, y] = wb1[:, y]

    factor = scale * math.log2(math.e)
    n_pairs = slots // 2
    n_chunks = 4
    per = n_pairs // n_chunks
    n_tok = per * 2
    lsum = jnp.zeros((heads, seqs), F32)
    for c in range(n_chunks):
        for j in range(per):
            i = c * per + j
            top = jnp.where(low, mrow[owner_of(2 * i)], mrow[owner_of(2 * i + 1)])
            live = jnp.max(fills[i], axis=0, keepdims=True) > 0.0
            p = jnp.where(live, jnp.exp2((sc[i] - top) * factor), 0.0).astype(BF16)
            p16 = p.reshape(heads // 16, 16, 128)
            for b in range(seqs):
                probs[b * heads : (b + 1) * heads, j * 128 : (j + 1) * 128] = (
                    p16 * maskt[i, b][None]
                ).reshape(heads, 128)
            lsum += dot(p, maskl[i], NT)
        part = dot(
            probs[...], lat[c * n_tok : (c + 1) * n_tok].reshape(n_tok * page, width), NN
        )
        acc[...] = part if c == 0 else acc[...] + part
        if c == 2:
            arrive(max1)
            top_x = mtile[...]
            for k in hops:
                top_x = jnp.maximum(top_x, mx[to_x(k)])
            mt2[...] = top_x
            max2 = [send(16, k, mt2, my2.at[y], at_y(k)) for k in hops]

    arrive(max1y)
    top_x = mt2[...]
    top_y = mtile[...]
    for k in hops:
        top_y = jnp.maximum(top_y, my[to_y(k)])

    tiles = hw // 128

    def every(ref, start, count):
        return jnp.concatenate(
            [ref[t, pl.ds(start, count, stride=side), :] for t in range(tiles)], axis=1
        ).astype(BF16)

    def put(ref, b, rows):
        for t in range(tiles):
            ref[t, b * side : (b + 1) * side, :] = rows[:, 128 * t : 128 * (t + 1)]

    def column(tile, b):
        return jnp.sum(
            jnp.where(diag, jnp.broadcast_to(tile[b : b + 1], (heads, 128)), 0.0),
            axis=1,
            keepdims=True,
        )

    for b in range(seqs):
        f0 = jnp.exp2((mrow[b] - column(top_x, b)) * factor)
        lrow[b] = f0 * lsum[:, b : b + 1]
        rows = acc[b * heads : (b + 1) * heads, :hw] * f0[:, :1]
        sx[:, b] = rows.astype(BF16).reshape(side, side, hw)
    sum1 = [send(8, k, sx.at[to_x(k)], rx.at[x], at_x(k)) for k in hops]
    for b in range(seqs):
        f1 = jnp.exp2((mrow[b] - column(top_y, b)) * factor)
        rows = acc[b * heads : (b + 1) * heads, hw:]
        for t in range(tiles):
            stage[t, b * heads : (b + 1) * heads, :] = (
                rows[:, 128 * t : 128 * (t + 1)] * f1
            )
    for b in range(seqs):
        for i in range(side):
            sy[i, b] = every(stage, b * heads + i, side)
    sum2 = [send(9, k, sy.at[to_y(k)], ry.at[y], at_y(k)) for k in hops]
    ltile[...] = to_lanes(lrow)
    tot1 = [send(10, k, ltile, lx.at[x], at_x(k)) for k in hops]

    arrive(max2)
    top = top_x
    for k in hops:
        top = jnp.maximum(top, my2[to_y(k)])
    shrink_x = jnp.exp2((top_x - top) * factor)
    shrink_y = jnp.exp2((top_y - top) * factor)
    row8 = lax.broadcasted_iota(jnp.int32, (side, 128), 0)
    lane_of = lax.broadcasted_iota(jnp.int32, (side, 128), 1)

    def pick(tile, b, which):
        return jnp.sum(
            jnp.where(lane_of == which, jnp.broadcast_to(tile[b : b + 1], (side, 128)), 0.0),
            axis=1,
            keepdims=True,
        )

    arrive(sum1)
    for b in range(seqs):
        rows = sx[x, b].astype(F32)
        for k in hops:
            rows += rx[to_x(k), b].astype(F32)
        put(r0, b, rows * pick(shrink_x, b, x * side + row8))
    for i in range(side):
        s2y[i] = every(r0, i, seqs)
    fin1 = [send(11, k, s2y.at[to_y(k)], r2y.at[y], at_y(k)) for k in hops]
    arrive(sum2)
    for b in range(seqs):
        rows = sy[y, b].astype(F32)
        for k in hops:
            rows += ry[to_y(k), b].astype(F32)
        put(r1, b, rows * pick(shrink_y, b, row8 * side + y))
    for i in range(side):
        s2x[i] = every(r1, i, seqs)
    fin2 = [send(12, k, s2x.at[to_x(k)], r2x.at[x], at_x(k)) for k in hops]
    arrive(tot1)
    total = ltile[...]
    for k in hops:
        total += lx[to_x(k)]
    lt2[...] = total * shrink_x
    tot2 = [send(13, k, lt2, ly.at[y], at_y(k)) for k in hops]

    arrive(fin1)
    att0 = s2y[y].astype(F32)
    for k in hops:
        att0 += r2y[to_y(k)].astype(F32)
    arrive(fin2)
    att1 = s2x[x].astype(F32)
    for k in hops:
        att1 += r2x[to_x(k)].astype(F32)
    arrive(tot2)
    total = lt2[...]
    for k in hops:
        total += ly[to_y(k)]
    total = jnp.sum(jnp.where(lane8 == me, total, 0.0), axis=1, keepdims=True)
    attention = (jnp.concatenate([att0, att1], axis=1) / total).astype(BF16)

    arrive(up2)
    value = dot(attention, wb2[...].reshape(width, wb2.shape[-1]), NN).astype(BF16)
    vals[x, y] = value
    val1 = [send(14, k, vals.at[x, y], vals.at[x, y], at_y(k)) for k in hops]
    wout_copy.wait()
    arrive(val1)
    val2 = {k: send(15, k, vals.at[x], vals.at[x], at_x(k)) for k in hops}
    block = side * vals.shape[-1]

    def project(i):
        flat = jnp.concatenate([vals[i, j] for j in range(side)], axis=1)
        start = pl.multiple_of(i * block, block)
        return dot(flat, wout[:, pl.ds(start, block)], NT)

    partial = project(x)
    for k in near:
        val2[k].wait_recv()
        partial += project(to_x(side - k))
    width_out = partial.shape[1]
    part_send[:, :width_out] = partial
    swap = pltpu.make_async_remote_copy(
        src_ref=part_send,
        dst_ref=part_recv,
        send_sem=mp_sem.at[0],
        recv_sem=mp_sem.at[1],
        device_id={"mp": 1 - mp},
        device_id_type=pl.DeviceIdType.MESH,
    )
    swap.start()
    swap.wait()
    both = partial + part_recv[:, :width_out]
    n_out = out.shape[1]
    out[...] = jnp.where(mp == 0, both[:, :n_out], both[:, n_out:]).astype(BF16)
    for copy in started:
        copy.wait_send()


def local(
    latent_cache, rope_cache, q_nope, q_rope, w_uk, value_up_weight, w_out, page_table, lengths
):
    slots, page, width = latent_cache.shape
    seqs, heads, nope = q_nope.shape
    cols, vdim = value_up_weight.shape[1:]
    side = math.isqrt(lax.axis_size("seq"))
    scale = (nope + q_rope.shape[2]) ** (-0.5)
    n_out = w_out.shape[1] // lax.axis_size("mp")
    half = seqs * heads // 2
    hw = width // 2
    chunk = slots * page // 4
    pitch = page + 4
    vm = pltpu.VMEM
    anywhere = pl.BlockSpec(memory_space=pl.ANY)
    in_vmem = pl.BlockSpec(memory_space=pltpu.VMEM)
    scratch = [
        vm(q_nope.shape, BF16),
        vm(q_rope.shape, BF16),
        vm((heads, cols, nope), BF16),
        vm(value_up_weight.shape, BF16),
        vm(page_table.shape, jnp.int32),
        pltpu.SMEM(lengths.shape, jnp.int32),
        vm((slots, page, width), BF16),
        vm(rope_cache.shape, BF16),
        vm((w_out.shape[1], w_out.shape[0]), BF16),
        vm((slots * pitch + page, 128), F32),
        vm((slots * page, 128), BF16),
        vm((seqs, heads, width + 128), BF16),
        vm((side, side, cols, half), BF16),
        vm((side, side, cols, half), BF16),
        vm((side, side, cols, vdim), BF16),
        vm((side, side, cols, vdim), BF16),
        vm((slots // 2, seqs, 128), F32),
        vm((seqs, 128), jnp.int32),
        pltpu.SMEM((seqs, 128), jnp.int32),
        vm((slots // 2, heads, 128), F32),
        vm((seqs, heads, 128), F32),
        vm((seqs, heads, 128), F32),
        vm((seqs, heads, 128), F32),
        vm((seqs * heads, chunk), BF16),
        vm((seqs * heads, width), F32),
        vm((slots // 2, seqs, 16, 128), BF16),
        vm((slots // 2, seqs, 128), BF16),
        vm((seqs, 128), F32),
        vm((side, seqs, 128), F32),
        vm((seqs, 128), F32),
        vm((side, seqs, 128), F32),
        vm((side, seqs, 128), F32),
        vm((seqs, 128), F32),
        vm((side, seqs, 128), F32),
        vm((seqs, 128), F32),
        vm((side, seqs, 128), F32),
        vm((side, seqs, side, hw), BF16),
        vm((side, seqs, side, hw), BF16),
        vm((side, seqs, side, hw), BF16),
        vm((side, seqs, side, hw), BF16),
        vm((hw // 128, seqs * heads + side, 128), F32),
        vm((hw // 128, seqs * side + side, 128), F32),
        vm((hw // 128, seqs * side + side, 128), F32),
        vm((side, seqs, hw), BF16),
        vm((side, seqs, hw), BF16),
        vm((side, seqs, hw), BF16),
        vm((side, seqs, hw), BF16),
        vm((side, side, seqs, vdim), BF16),
        vm((seqs, 128), F32),
        vm((seqs, 128), F32),
        pltpu.SemaphoreType.DMA((12,)),
        pltpu.SemaphoreType.DMA,
        pltpu.SemaphoreType.DMA((17, side)),
        pltpu.SemaphoreType.DMA((17, side)),
        pltpu.SemaphoreType.DMA((2,)),
    ]
    return pl.pallas_call(
        functools.partial(kernel, side, scale),
        out_shape=jax.ShapeDtypeStruct((seqs, n_out), BF16),
        in_specs=[anywhere] * 9,
        out_specs=in_vmem,
        scratch_shapes=scratch,
        compiler_params=pltpu.CompilerParams(
            collective_id=0, has_side_effects=True, vmem_limit_bytes=60 * 1024 * 1024
        ),
        name="decode",
    )(
        q_nope,
        q_rope,
        jnp.swapaxes(w_uk, 1, 2),
        value_up_weight,
        page_table,
        lengths,
        latent_cache,
        rope_cache,
        jnp.swapaxes(w_out, 0, 1),
    )


def solution(mesh):
    return jax.shard_map(
        local,
        mesh=mesh,
        in_specs=(
            P(GROUPS_SEQ, None, None),
            P(GROUPS_SEQ, None),
            P("groups", "mp", None),
            P("groups", "mp", None),
            P("mp", None, "seq"),
            P("mp", "seq", None),
            P("mp", "seq"),
            P("groups", None),
            P("groups"),
        ),
        out_specs=P("groups", ("seq", "mp")),
        check_vma=False,
    )
```

```python
import functools
import math

import jax
import jax.numpy as jnp
from jax import lax
from jax.experimental import pallas as pl
from jax.experimental.pallas import tpu as pltpu
from jax.sharding import PartitionSpec as P

GROUPS_SEQ = ("groups", "seq")
NEG = -1e30
F32 = jnp.float32
BF16 = jnp.bfloat16
NT = (((1,), (1,)), ((), ()))
NN = (((1,), (0,)), ((), ()))


def dot(a, b, dims):
    return lax.dot_general(a, b, dims, preferred_element_type=F32)


def kernel(
    side,
    scale,
    q_nope_hbm,
    q_rope_hbm,
    w_uk_hbm,
    w_up_hbm,
    table_hbm,
    lengths_hbm,
    latent_hbm,
    rope_hbm,
    w_out_hbm,
    out,
    q_nope,
    q_rope,
    w_uk,
    w_up,
    table,
    lengths,
    lat,
    rope,
    wout,
    spread,
    keys,
    q_all,
    g0,
    g1,
    wb1,
    wb2,
    fills,
    owner_v,
    owner_s,
    sc,
    mrow,
    lrow,
    mrun,
    probs,
    acc,
    maskt,
    maskl,
    mtile,
    mx,
    mt2,
    my,
    my2,
    ltile,
    lx,
    lt2,
    ly,
    sx,
    sy,
    rx,
    ry,
    stage,
    r0,
    r1,
    s2y,
    s2x,
    r2y,
    r2x,
    vals,
    part_send,
    part_recv,
    load_sem,
    own_sem,
    send_sem,
    recv_sem,
    mp_sem,
):
    seqs, heads, nope = q_nope.shape
    slots, page, width = lat.shape
    half = seqs * heads // 2
    hw = width // 2
    me = lax.axis_index("seq")
    mp = lax.axis_index("mp")
    x, y = lax.div(me, side), lax.rem(me, side)
    hops = sorted(range(1, side), key=lambda k: -min(k, side - k))

    def to_x(k):
        return lax.rem(x + k, side)

    def to_y(k):
        return lax.rem(y + k, side)

    def at_x(k):
        return {"seq": to_x(k) * side + y}

    def at_y(k):
        return {"seq": x * side + to_y(k)}

    barrier = pltpu.get_barrier_semaphore()
    for k in hops:
        pl.semaphore_signal(barrier, inc=1, device_id=at_x(k), device_id_type=pl.DeviceIdType.MESH)
        pl.semaphore_signal(barrier, inc=1, device_id=at_y(k), device_id_type=pl.DeviceIdType.MESH)
    pl.semaphore_signal(
        barrier, inc=1, device_id={"mp": 1 - mp}, device_id_type=pl.DeviceIdType.MESH
    )

    loads = []
    n_cut = 4
    cut = slots // n_cut

    def load(src, dst):
        copy = pltpu.make_async_copy(src, dst, load_sem.at[len(loads)])
        copy.start()
        loads.append(copy)
        return copy

    query_copies = [load(q_nope_hbm, q_nope), load(w_uk_hbm, w_uk)]
    rope_copy = load(rope_hbm, rope)
    table_copies = [load(table_hbm, table), load(lengths_hbm, lengths)]
    side_copies = [load(q_rope_hbm, q_rope), load(w_up_hbm, w_up)]
    lat_copies = [
        load(latent_hbm.at[pl.ds(i * cut, cut)], lat.at[pl.ds(i * cut, cut)])
        for i in range(n_cut)
    ]
    wout_copy = load(w_out_hbm, wout)

    started = []

    def send(phase, k, src, dst, device):
        copy = pltpu.make_async_remote_copy(
            src_ref=src,
            dst_ref=dst,
            send_sem=send_sem.at[phase, k],
            recv_sem=recv_sem.at[phase, k],
            device_id=device,
            device_id_type=pl.DeviceIdType.MESH,
        )
        copy.start()
        started.append(copy)
        return copy

    def arrive(copies):
        for copy in copies:
            copy.wait_recv()

    for copy in query_copies:
        copy.wait()

    cols = w_uk.shape[1]
    wide = dot(
        w_uk[...].reshape(heads * cols, nope), q_nope[...].reshape(seqs * heads, nope), NT
    ).reshape(heads, cols, seqs * heads)
    row_head = lax.broadcasted_iota(jnp.int32, wide.shape, 0)
    col_head = lax.rem(lax.broadcasted_iota(jnp.int32, wide.shape, 2), heads)
    q_part = jnp.sum(jnp.where(row_head == col_head, wide, 0.0), axis=0).astype(BF16)
    g0[x, y] = q_part[:, :half]
    g1[y, x] = q_part[:, half:]

    pl.semaphore_wait(barrier, 2 * (side - 1) + 1)

    near = hops[::-1]
    first0 = {k: send(0, k, g0.at[x, y], g0.at[x, y], at_y(k)) for k in hops}
    first1 = {k: send(1, k, g1.at[y, x], g1.at[y, x], at_x(k)) for k in hops}

    def forward(phase, k, piece, device):
        return pltpu.make_async_remote_copy(
            src_ref=piece,
            dst_ref=piece,
            send_sem=send_sem.at[phase, k],
            recv_sem=recv_sem.at[phase, k],
            device_id=device,
            device_id_type=pl.DeviceIdType.MESH,
        )

    def pass_on(row, col):
        for k in hops:
            forward(2, k, g0.at[x, row], at_x(k)).start()
            forward(3, k, g1.at[y, col], at_y(k)).start()

    second0 = [forward(2, k, g0.at[x], at_x(k)) for k in hops]
    second1 = [forward(3, k, g1.at[y], at_y(k)) for k in hops]
    started.extend(second0 + second1)
    pass_on(y, x)

    lane = lax.broadcasted_iota(jnp.int32, (1, 128), 1)
    low = lane < page
    pitch = spread.shape[0] // slots
    rope_copy.wait()

    def spread_pair(c, carry):
        z = rope[:, pl.ds(pl.multiple_of(c * 128, 128), 128)].astype(F32)
        spread[pl.ds(2 * c, slots, stride=pitch), :] = jnp.where(low, z, 0.0)
        spread[pl.ds(2 * c + 1, slots, stride=pitch), :] = jnp.where(low, 0.0, z)
        return carry

    lax.fori_loop(0, rope.shape[1] // 128, spread_pair, 0)

    def owner_of(slot):
        return jnp.clip(owner_s[0, slot], 0, seqs - 1)

    for copy in table_copies:
        copy.wait()

    row = lax.broadcasted_iota(jnp.int32, (seqs, 1), 0)
    length = jnp.zeros((seqs, 1), jnp.int32)
    for b in range(seqs):
        length = jnp.where(row == b, lengths[b], length)
    pages = lax.broadcasted_iota(jnp.int32, table.shape, 1)
    tokens = jnp.clip(length - page * pages, 0, page).astype(F32)
    relative = table[...] - me * slots
    lane8 = lax.broadcasted_iota(jnp.int32, (seqs, 128), 1)
    token = lax.rem(lane8, page).astype(F32)

    def fill_pair(i, owner):
        f0 = jnp.max(jnp.where(relative == 2 * i, tokens, 0.0), axis=1, keepdims=True)
        f1 = jnp.max(jnp.where(relative == 2 * i + 1, tokens, 0.0), axis=1, keepdims=True)
        fills[i] = jnp.where(lane8 < page, f0, f1) - token
        owner = jnp.where((lane8 == 2 * i) & (f0 > 0.0), row, owner)
        return jnp.where((lane8 == 2 * i + 1) & (f1 > 0.0), row, owner)

    owner = lax.fori_loop(
        0, slots // 2, fill_pair, jnp.zeros((seqs, 128), jnp.int32), unroll=8
    )
    owner_v[...] = jnp.broadcast_to(
        jnp.max(owner.astype(F32), axis=0, keepdims=True), owner.shape
    ).astype(jnp.int32)
    own_copy = pltpu.make_async_copy(owner_v, owner_s, own_sem)
    own_copy.start()

    for k in near:
        first0[k].wait_recv()
        first1[k].wait_recv()
        pass_on(to_y(side - k), to_x(side - k))
    def pack_rows(s, carry):
        keys[pl.ds(pl.multiple_of(s * page, page), page), :] = spread[
            pl.ds(s * pitch, page), :
        ].astype(BF16)
        return carry

    lax.fori_loop(0, slots, pack_rows, 0, unroll=4)

    def mask_pair(i, carry):
        live = jnp.where(fills[i] > 0.0, 1.0, 0.0)
        maskl[i] = live.astype(BF16)
        for b in range(seqs):
            maskt[i, b] = jnp.broadcast_to(live[b : b + 1], (16, 128)).astype(BF16)
        return carry

    lax.fori_loop(0, slots // 2, mask_pair, 0, unroll=4)

    for copy in side_copies:
        copy.wait()
    for b in range(seqs):
        q_all[b, :, width:] = jnp.concatenate([q_rope[b], q_rope[b]], axis=-1)

    own_copy.wait()
    arrive(second0)
    arrive(second1)

    up1 = [
        send(4, k, w_up.at[pl.ds(to_x(k) * side, side)], wb1.at[x], at_x(k)) for k in hops
    ]
    wb1[x] = w_up[pl.ds(x * side, side)]

    eye = (
        lax.broadcasted_iota(jnp.int32, (half, half), 0)
        == lax.broadcasted_iota(jnp.int32, (half, half), 1)
    ).astype(BF16)
    columns0 = g0[...].reshape(width, half)
    columns1 = jnp.concatenate(
        [g1[:, i].reshape(side * cols, half) for i in range(side)], axis=0
    )
    for i, columns in enumerate((columns0, columns1)):
        rows = dot(eye, columns, NT).astype(BF16).reshape(seqs // 2, heads, width)
        q_all[i * (seqs // 2) : (i + 1) * (seqs // 2), :, :width] = rows

    for copy in lat_copies:
        copy.wait()

    def score_group(g, carry):
        picked = jnp.concatenate([q_all[owner_of(4 * g + j)] for j in range(4)], axis=0)
        tok = lat[pl.ds(g * 4, 4)].reshape(4 * page, width)
        rot = keys[pl.ds(pl.multiple_of(g * 4 * page, 4 * page), 4 * page), :]
        s = dot(picked[:, :width], tok, NT) + dot(picked[:, width:], rot, NT)
        blocks = []
        for j in range(2):
            r, c = 2 * heads * j, 2 * page * j
            block = jnp.where(
                low,
                s[r : r + heads, c : c + 2 * page],
                s[r + heads : r + 2 * heads, c : c + 2 * page],
            )
            sc[2 * g + j] = block
            blocks.append(block)
        for b in range(seqs):
            m = mrun[b]
            for j in range(2):
                m = jnp.maximum(m, jnp.where(fills[2 * g + j, b : b + 1] > 0.0, blocks[j], NEG))
            mrun[b] = m
        return carry

    mrun[...] = jnp.full(mrun.shape, NEG, F32)
    lax.fori_loop(0, slots // 4, score_group, 0, unroll=8)
    for b in range(seqs):
        mrow[b] = jnp.broadcast_to(jnp.max(mrun[b], axis=1, keepdims=True), (heads, 128))

    head_lane = lax.broadcasted_iota(jnp.int32, (heads, 128), 1)
    head_row = lax.broadcasted_iota(jnp.int32, (heads, 128), 0)
    diag = head_lane == head_row

    def to_lanes(ref):
        return jnp.concatenate(
            [
                jnp.sum(jnp.where(diag, ref[b], 0.0), axis=0, keepdims=True)
                for b in range(seqs)
            ],
            axis=0,
        )

    mtile[...] = to_lanes(mrow)
    max1 = [send(6, k, mtile, mx.at[x], at_x(k)) for k in hops]
    max1y = [send(7, k, mtile, my.at[y], at_y(k)) for k in hops]
    arrive(up1)
    up2 = [send(5, k, wb1.at[:, to_y(k)], wb2.at[:, y], at_y(k)) for k in hops]
    wb2[:, y] = wb1[:, y]

    factor = scale * math.log2(math.e)
    n_pairs = slots // 2
    n_chunks = 4
    per = n_pairs // n_chunks
    n_tok = per * 2
    lsum = jnp.zeros((heads, seqs), F32)
    for c in range(n_chunks):
        for j in range(per):
            i = c * per + j
            top = jnp.where(low, mrow[owner_of(2 * i)], mrow[owner_of(2 * i + 1)])
            live = jnp.max(fills[i], axis=0, keepdims=True) > 0.0
            p = jnp.where(live, jnp.exp2((sc[i] - top) * factor), 0.0).astype(BF16)
            p16 = p.reshape(heads // 16, 16, 128)
            for b in range(seqs):
                probs[b * heads : (b + 1) * heads, j * 128 : (j + 1) * 128] = (
                    p16 * maskt[i, b][None]
                ).reshape(heads, 128)
            lsum += dot(p, maskl[i], NT)
        part = dot(
            probs[...], lat[c * n_tok : (c + 1) * n_tok].reshape(n_tok * page, width), NN
        )
        acc[...] = part if c == 0 else acc[...] + part
        if c == 2:
            arrive(max1)
            top_x = mtile[...]
            for k in hops:
                top_x = jnp.maximum(top_x, mx[to_x(k)])
            mt2[...] = top_x
            max2 = [send(16, k, mt2, my2.at[y], at_y(k)) for k in hops]

    arrive(max1y)
    top_x = mt2[...]
    top_y = mtile[...]
    for k in hops:
        top_y = jnp.maximum(top_y, my[to_y(k)])

    tiles = hw // 128

    def every(ref, start, count):
        return jnp.concatenate(
            [ref[t, pl.ds(start, count, stride=side), :] for t in range(tiles)], axis=1
        ).astype(BF16)

    def put(ref, b, rows):
        for t in range(tiles):
            ref[t, b * side : (b + 1) * side, :] = rows[:, 128 * t : 128 * (t + 1)]

    def column(tile, b):
        return jnp.sum(
            jnp.where(diag, jnp.broadcast_to(tile[b : b + 1], (heads, 128)), 0.0),
            axis=1,
            keepdims=True,
        )

    for b in range(seqs):
        f0 = jnp.exp2((mrow[b] - column(top_x, b)) * factor)
        lrow[b] = f0 * lsum[:, b : b + 1]
        rows = acc[b * heads : (b + 1) * heads, :hw] * f0[:, :1]
        sx[:, b] = rows.astype(BF16).reshape(side, side, hw)
    sum1 = [send(8, k, sx.at[to_x(k)], rx.at[x], at_x(k)) for k in hops]
    for b in range(seqs):
        f1 = jnp.exp2((mrow[b] - column(top_y, b)) * factor)
        rows = acc[b * heads : (b + 1) * heads, hw:]
        for t in range(tiles):
            stage[t, b * heads : (b + 1) * heads, :] = (
                rows[:, 128 * t : 128 * (t + 1)] * f1
            )
    for b in range(seqs):
        for i in range(side):
            sy[i, b] = every(stage, b * heads + i, side)
    sum2 = [send(9, k, sy.at[to_y(k)], ry.at[y], at_y(k)) for k in hops]
    ltile[...] = to_lanes(lrow)
    tot1 = [send(10, k, ltile, lx.at[x], at_x(k)) for k in hops]

    arrive(max2)
    top = top_x
    for k in hops:
        top = jnp.maximum(top, my2[to_y(k)])
    shrink_x = jnp.exp2((top_x - top) * factor)
    shrink_y = jnp.exp2((top_y - top) * factor)
    row8 = lax.broadcasted_iota(jnp.int32, (side, 128), 0)
    lane_of = lax.broadcasted_iota(jnp.int32, (side, 128), 1)

    def pick(tile, b, which):
        return jnp.sum(
            jnp.where(lane_of == which, jnp.broadcast_to(tile[b : b + 1], (side, 128)), 0.0),
            axis=1,
            keepdims=True,
        )

    arrive(sum1)
    for b in range(seqs):
        rows = sx[x, b].astype(F32)
        for k in hops:
            rows += rx[to_x(k), b].astype(F32)
        put(r0, b, rows * pick(shrink_x, b, x * side + row8))
    for i in range(side):
        s2y[i] = every(r0, i, seqs)
    fin1 = [send(11, k, s2y.at[to_y(k)], r2y.at[y], at_y(k)) for k in hops]
    arrive(sum2)
    for b in range(seqs):
        rows = sy[y, b].astype(F32)
        for k in hops:
            rows += ry[to_y(k), b].astype(F32)
        put(r1, b, rows * pick(shrink_y, b, row8 * side + y))
    for i in range(side):
        s2x[i] = every(r1, i, seqs)
    fin2 = [send(12, k, s2x.at[to_x(k)], r2x.at[x], at_x(k)) for k in hops]
    arrive(tot1)
    total = ltile[...]
    for k in hops:
        total += lx[to_x(k)]
    lt2[...] = total * shrink_x
    tot2 = [send(13, k, lt2, ly.at[y], at_y(k)) for k in hops]

    arrive(fin1)
    att0 = s2y[y].astype(F32)
    for k in hops:
        att0 += r2y[to_y(k)].astype(F32)
    arrive(fin2)
    att1 = s2x[x].astype(F32)
    for k in hops:
        att1 += r2x[to_x(k)].astype(F32)
    arrive(tot2)
    total = lt2[...]
    for k in hops:
        total += ly[to_y(k)]
    total = jnp.sum(jnp.where(lane8 == me, total, 0.0), axis=1, keepdims=True)
    attention = (jnp.concatenate([att0, att1], axis=1) / total).astype(BF16)

    arrive(up2)
    value = dot(attention, wb2[...].reshape(width, wb2.shape[-1]), NN).astype(BF16)
    vals[x, y] = value
    val1 = [send(14, k, vals.at[x, y], vals.at[x, y], at_y(k)) for k in hops]
    wout_copy.wait()
    arrive(val1)
    val2 = {k: send(15, k, vals.at[x], vals.at[x], at_x(k)) for k in hops}
    block = side * vals.shape[-1]

    def project(i):
        flat = jnp.concatenate([vals[i, j] for j in range(side)], axis=1)
        start = pl.multiple_of(i * block, block)
        return dot(flat, wout[:, pl.ds(start, block)], NT)

    partial = project(x)
    for k in near:
        val2[k].wait_recv()
        partial += project(to_x(side - k))
    width_out = partial.shape[1]
    part_send[:, :width_out] = partial
    swap = pltpu.make_async_remote_copy(
        src_ref=part_send,
        dst_ref=part_recv,
        send_sem=mp_sem.at[0],
        recv_sem=mp_sem.at[1],
        device_id={"mp": 1 - mp},
        device_id_type=pl.DeviceIdType.MESH,
    )
    swap.start()
    swap.wait()
    both = partial + part_recv[:, :width_out]
    n_out = out.shape[1]
    out[...] = jnp.where(mp == 0, both[:, :n_out], both[:, n_out:]).astype(BF16)
    for copy in started:
        copy.wait_send()


def local(
    latent_cache, rope_cache, q_nope, q_rope, w_uk, value_up_weight, w_out, page_table, lengths
):
    slots, page, width = latent_cache.shape
    seqs, heads, nope = q_nope.shape
    cols, vdim = value_up_weight.shape[1:]
    side = math.isqrt(lax.axis_size("seq"))
    scale = (nope + q_rope.shape[2]) ** (-0.5)
    n_out = w_out.shape[1] // lax.axis_size("mp")
    half = seqs * heads // 2
    hw = width // 2
    chunk = slots * page // 4
    pitch = page + 4
    vm = pltpu.VMEM
    anywhere = pl.BlockSpec(memory_space=pl.ANY)
    in_vmem = pl.BlockSpec(memory_space=pltpu.VMEM)
    scratch = [
        vm(q_nope.shape, BF16),
        vm(q_rope.shape, BF16),
        vm((heads, cols, nope), BF16),
        vm(value_up_weight.shape, BF16),
        vm(page_table.shape, jnp.int32),
        pltpu.SMEM(lengths.shape, jnp.int32),
        vm((slots, page, width), BF16),
        vm(rope_cache.shape, BF16),
        vm((w_out.shape[1], w_out.shape[0]), BF16),
        vm((slots * pitch + page, 128), F32),
        vm((slots * page, 128), BF16),
        vm((seqs, heads, width + 128), BF16),
        vm((side, side, cols, half), BF16),
        vm((side, side, cols, half), BF16),
        vm((side, side, cols, vdim), BF16),
        vm((side, side, cols, vdim), BF16),
        vm((slots // 2, seqs, 128), F32),
        vm((seqs, 128), jnp.int32),
        pltpu.SMEM((seqs, 128), jnp.int32),
        vm((slots // 2, heads, 128), F32),
        vm((seqs, heads, 128), F32),
        vm((seqs, heads, 128), F32),
        vm((seqs, heads, 128), F32),
        vm((seqs * heads, chunk), BF16),
        vm((seqs * heads, width), F32),
        vm((slots // 2, seqs, 16, 128), BF16),
        vm((slots // 2, seqs, 128), BF16),
        vm((seqs, 128), F32),
        vm((side, seqs, 128), F32),
        vm((seqs, 128), F32),
        vm((side, seqs, 128), F32),
        vm((side, seqs, 128), F32),
        vm((seqs, 128), F32),
        vm((side, seqs, 128), F32),
        vm((seqs, 128), F32),
        vm((side, seqs, 128), F32),
        vm((side, seqs, side, hw), BF16),
        vm((side, seqs, side, hw), BF16),
        vm((side, seqs, side, hw), BF16),
        vm((side, seqs, side, hw), BF16),
        vm((hw // 128, seqs * heads + side, 128), F32),
        vm((hw // 128, seqs * side + side, 128), F32),
        vm((hw // 128, seqs * side + side, 128), F32),
        vm((side, seqs, hw), BF16),
        vm((side, seqs, hw), BF16),
        vm((side, seqs, hw), BF16),
        vm((side, seqs, hw), BF16),
        vm((side, side, seqs, vdim), BF16),
        vm((seqs, 128), F32),
        vm((seqs, 128), F32),
        pltpu.SemaphoreType.DMA((12,)),
        pltpu.SemaphoreType.DMA,
        pltpu.SemaphoreType.DMA((17, side)),
        pltpu.SemaphoreType.DMA((17, side)),
        pltpu.SemaphoreType.DMA((2,)),
    ]
    return pl.pallas_call(
        functools.partial(kernel, side, scale),
        out_shape=pltpu.VMEM((seqs, n_out), BF16),
        in_specs=[anywhere] * 9,
        out_specs=in_vmem,
        scratch_shapes=scratch,
        compiler_params=pltpu.CompilerParams(
            collective_id=0, has_side_effects=True, vmem_limit_bytes=60 * 1024 * 1024
        ),
        name="decode",
    )(
        q_nope,
        q_rope,
        jnp.swapaxes(w_uk, 1, 2),
        value_up_weight,
        page_table,
        lengths,
        latent_cache,
        rope_cache,
        jnp.swapaxes(w_out, 0, 1),
    )


def solution(mesh):
    return jax.shard_map(
        local,
        mesh=mesh,
        in_specs=(
            P(GROUPS_SEQ, None, None),
            P(GROUPS_SEQ, None),
            P("groups", "mp", None),
            P("groups", "mp", None),
            P("mp", None, "seq"),
            P("mp", "seq", None),
            P("mp", "seq"),
            P("groups", None),
            P("groups"),
        ),
        out_specs=P("groups", ("seq", "mp")),
        check_vma=False,
    )
```
